32 devices in a mesh: gx: 8 (over z, core), gy: 2 (over y), gz: 2 (over x).
Axes of the slice: x: 2, y: 2, z: 4, core: 2. Of those that a mesh axis runs over, the one named last changes fastest.
Arguments:
- volume: float32 [128, 128, 256], P('gx', 'gy', 'gz'), may hold values from -6 to 6
- weights: float32 [64, 8, 128], P(None, None, 'gx'), may hold values from -0.1875 to 0.1875
- offsets: int32 [64, 8], P(None, 'gx'), may hold values from 0 to 57, as said below
- measured: float32 [64, 128, 256], P('gx', 'gy', 'gz'), may hold values from -6 to 6
Outputs:
- gradient: float32 [128, 128, 256], P('gx', 'gy', 'gz')
- residual: float32 [64, 128, 256], P('gx', 'gy', 'gz')
- misfit: float32 [], replicated
The draws below stay inside these ranges and needn't reach their ends.
Inputs may be any that keep to these rules, and one draw needn't show every extreme that they name: offsets[a, b] shifts angle a on brick b; the values 0 and 57 both occur.
All inputs are finite; a program needn't handle non-finite values.
Results may differ from the reference program's by a relative error of at most 0.0003.
Values sent between devices are 32-bit elements; how exact they have to be, the bound alone decides.
A program may use at most 64 MiB of HBM per device.

```python
import jax
import jax.numpy as jnp
from jax import lax

CX = 16
CY = 64
ANGLES = 64
TAPS = 8
BRICKS_X = 8
NX = 128
NY = 128
NZ = 256
N_GX = 8


def draw_offsets(key, part):
    first, second, third = jax.random.split(jax.random.fold_in(key, 17), 3)
    count = ANGLES * BRICKS_X
    values = jax.random.randint(first, (count,), 0, CY - TAPS + 2)
    high_pos = jax.random.randint(second, (), 0, count)
    low_pos = (high_pos + 1 + jax.random.randint(third, (), 0, count - 1)) % count
    values = values.at[high_pos].set(CY - TAPS + 1)
    values = values.at[low_pos].set(0)
    return values.reshape(ANGLES, BRICKS_X).astype(jnp.int32)


def levels(stream_key, extent, shards, least, largest):
    loudness, own = 1.0, jax.random.fold_in(stream_key, 6)
    for axis_at, parts in shards:
        draws = jnp.exp(jax.random.uniform(jax.random.fold_in(own, axis_at), (parts,), jnp.float32, least / len(shards), largest / len(shards)))
        loudness = loudness * jnp.repeat(draws, extent[axis_at] // parts).reshape([-1 if axis == axis_at else 1 for axis in range(len(extent))])
    return loudness


def normal_values(own_key, dims, scale, reach, shards=(), dtype=jnp.bfloat16):
    drawn = scale * jax.random.normal(own_key, dims, jnp.float32)
    if shards:
        drawn = drawn * levels(own_key, dims, shards, -0.22, 0.18)
    return jnp.clip(drawn, -reach, reach).astype(dtype)


def setup_inputs(seed: int = 0) -> dict:
    key_list = jax.random.split(jax.random.key(seed), 5)
    volume = normal_values(key_list[0], (NX, NY, NZ), 1.0, 6.0, ((0, 8), (1, 2), (2, 2)), jnp.float32)
    weights = normal_values(key_list[1], (ANGLES, TAPS, NX), (NX * TAPS) ** -0.5, 0.1875, ((2, 8),), jnp.float32)
    offsets = draw_offsets(jax.random.fold_in(key_list[4], 71), 0)
    measured = normal_values(key_list[3], (ANGLES, NY, NZ), 1.0, 6.0, ((0, 8), (1, 2), (2, 2)), jnp.float32)
    return {"volume": volume, "weights": weights, "offsets": offsets, "measured": measured}


def project_brick(vol_brick, w_brick, off_brick):
    wblk = w_brick.reshape(ANGLES // 8, 8, TAPS, CX)
    oblk = off_brick.reshape(ANGLES // 8, 8)

    def one_block(args):
        wb, ob = args
        spread = jnp.einsum('adc,cyz->adyz', wb, vol_brick, precision=lax.Precision.HIGHEST)
        padded = jnp.pad(spread, ((0, 0), (0, 0), (0, CY), (0, 0)))

        def per_angle(plane, shift):
            window = lax.dynamic_slice_in_dim(plane, shift.astype(jnp.int32), NY + TAPS - 1, 1)
            total = jnp.zeros((NY, NZ), jnp.float32)
            for tap in range(TAPS):
                total = total + window[tap, tap:tap + NY]
            return total

        return jax.vmap(per_angle)(padded, ob)

    return lax.map(one_block, (wblk, oblk)).reshape(ANGLES, NY, NZ)


def back_brick(resid, w_brick, off_brick):
    padded = jnp.pad(resid, ((0, 0), (CY, 0), (0, 0)))
    wblk = w_brick.reshape(ANGLES // 8, 8, TAPS, CX)
    oblk = off_brick.reshape(ANGLES // 8, 8)
    rblk = padded.reshape(ANGLES // 8, 8, NY + CY, NZ)

    def one_block(grad, args):
        wb, ob, rb = args

        def per_angle(plane, shift):
            start = (CY - shift - (TAPS - 1)).astype(jnp.int32)
            window = lax.dynamic_slice_in_dim(plane, start, NY + TAPS - 1, 0)
            return jnp.stack([window[TAPS - 1 - tap:TAPS - 1 - tap + NY] for tap in range(TAPS)])

        sheared = jax.vmap(per_angle)(rb, ob)
        grad = grad + jnp.einsum('adc,adyz->cyz', wb, sheared, precision=lax.Precision.HIGHEST)
        return grad, None

    grad, unused = lax.scan(one_block, jnp.zeros((CX, NY, NZ), jnp.float32), (wblk, oblk, rblk))
    return grad


def reference(volume, weights, offsets, measured):
    vols = volume.reshape(N_GX, CX, NY, NZ)
    wts = weights.reshape(ANGLES, TAPS, N_GX, CX).transpose(2, 0, 1, 3)
    offs = offsets.T

    def accumulate(total, args):
        vb, wb, ob = args
        return total + project_brick(vb, wb, ob), None

    projection, unused = lax.scan(accumulate, jnp.zeros((ANGLES, NY, NZ), jnp.float32), (vols, wts, offs))
    residual = projection - measured
    misfit = jnp.sum(residual * residual) / (ANGLES * NY * NZ)

    def backward(args):
        wb, ob = args
        return back_brick(residual, wb, ob)

    gradient = lax.map(backward, (wts, offs)).reshape(NX, NY, NZ)
    return gradient, residual, misfit
```

```python
import functools

import jax
import jax.numpy as jnp
from jax import lax
from jax.experimental import pallas as pl
from jax.experimental.pallas import tpu as pltpu
from jax.sharding import PartitionSpec as P

SUB = 8
WIN = 16


def passed_along(x, axis, by):
    count = lax.axis_size(axis)
    pairs = [(i, i + by) for i in range(count) if 0 <= i + by < count]
    return lax.ppermute(x, axis, pairs)


def split(x):
    hi = x.astype(jnp.bfloat16)
    lo = (x - hi.astype(jnp.float32)).astype(jnp.bfloat16)
    return hi, lo


def toeplitz(flat):
    lead, lanes = flat.shape
    wide = jnp.broadcast_to(flat[:, None, :], (lead, SUB, lanes))
    rolled = pltpu.roll(wide, 0, 2, stride=1, stride_axis=1)
    return rolled.reshape(lead * SUB, lanes)


def dot(x, y):
    return jnp.dot(x, y, preferred_element_type=jnp.float32)


def forward_kernel(off_ref, w_ref, vol_ref, halo_ref, part_ref, ext, q, thi, tlo):
    cols, rows, depth = vol_ref.shape
    angles = w_ref.shape[0]
    ext[:, :rows] = vol_ref[...]
    ext[:, rows : 2 * rows] = halo_ref[...]
    ext[:, 2 * rows :] = jnp.zeros((cols, SUB, depth), jnp.float32)
    thi[...], tlo[...] = split(toeplitz(w_ref[...]))

    def block(j, carry):
        at = pl.multiple_of(j * SUB, SUB)
        hi, lo = split(ext[:, pl.ds(at, WIN), :].reshape(cols * WIN, depth))
        both = dot(thi[...], jnp.concatenate([hi, lo], axis=1))
        res = both[:, :depth] + both[:, depth:] + dot(tlo[...], hi)
        q[:, pl.ds(at, SUB), :] = res.reshape(angles, SUB, depth)
        return carry

    lax.fori_loop(0, 2 * rows // SUB, block, 0)

    def shift(a, carry):
        part_ref[a] = q[a, pl.ds(off_ref[a], rows), :]
        return carry

    lax.fori_loop(0, angles, shift, 0, unroll=4)


def backward_kernel(off_ref, w_ref, res_ref, up_ref, own_ref, ext, thi, tlo, rhs):
    angles, rows, depth = res_ref.shape
    cols = w_ref.shape[0]
    taps = WIN - SUB
    ext[:, :rows] = jnp.zeros((angles, rows, depth), jnp.float32)
    ext[:, rows : 2 * rows] = res_ref[...]
    ext[:, 2 * rows :] = jnp.zeros((angles, rows + SUB, depth), jnp.float32)
    thi[...], tlo[...] = split(toeplitz(w_ref[...]))

    def block(j, out_ref, base):
        at = pl.multiple_of(j * SUB, SUB)

        def gather(a, carry):
            start = rows + base + j * SUB - (taps - 1) - off_ref[a]
            hi, lo = split(ext[a, pl.ds(start, WIN), :])
            to = pl.multiple_of(a * WIN, WIN)
            rhs[pl.ds(to, WIN), :depth] = hi
            rhs[pl.ds(to, WIN), depth:] = lo
            return carry

        lax.fori_loop(0, angles, gather, 0, unroll=8)
        both = dot(thi[...], rhs[...])
        res = both[:, :depth] + both[:, depth:] + dot(tlo[...], rhs[:, :depth])
        out_ref[:, pl.ds(at, SUB), :] = res.reshape(cols, SUB, depth)

    @pl.loop(0, rows // SUB)
    def _(j):
        block(j, up_ref, rows)

    @pl.loop(0, rows // SUB)
    def _(j):
        block(j, own_ref, 0)


VMEM = pl.BlockSpec(memory_space=pltpu.VMEM)
SMEM = pl.BlockSpec(memory_space=pltpu.SMEM)


def body(volume, weights, offsets, measured):
    cols, rows, depth = volume.shape
    angles, taps, _ = weights.shape
    shifts = offsets[:, 0]
    halo = passed_along(volume, "gy", -1)
    pad = ((0, 0), (0, 0), (0, WIN - taps))
    w_fwd = jnp.pad(weights.transpose(0, 2, 1), pad).reshape(angles, cols * WIN)
    w_bwd = jnp.pad(weights[:, ::-1].transpose(2, 0, 1), pad).reshape(cols, angles * WIN)
    f32, bf16 = jnp.float32, jnp.bfloat16
    partial_value = pl.pallas_call(
        forward_kernel,
        out_shape=jax.ShapeDtypeStruct((angles, rows, depth), f32),
        in_specs=[SMEM, VMEM, VMEM, VMEM],
        out_specs=VMEM,
        scratch_shapes=[
            pltpu.VMEM((cols, 2 * rows + SUB, depth), f32),
            pltpu.VMEM((angles, 2 * rows, depth), f32),
            pltpu.VMEM((angles * SUB, cols * WIN), bf16),
            pltpu.VMEM((angles * SUB, cols * WIN), bf16),
        ],
    )(shifts, w_fwd, volume, halo)
    summed = lax.psum_scatter(partial_value, "gx", scatter_dimension=0, tiled=True)
    resid_share = summed - measured
    resid_all = lax.all_gather(resid_share, "gx", axis=0, tiled=True)
    share = jax.ShapeDtypeStruct((cols, rows, depth), f32)
    upper, own = pl.pallas_call(
        backward_kernel,
        out_shape=[share, share],
        in_specs=[SMEM, VMEM, VMEM],
        out_specs=[VMEM, VMEM],
        scratch_shapes=[
            pltpu.VMEM((angles, 3 * rows + SUB, depth), f32),
            pltpu.VMEM((cols * SUB, angles * WIN), bf16),
            pltpu.VMEM((cols * SUB, angles * WIN), bf16),
            pltpu.VMEM((angles * WIN, 2 * depth), bf16),
        ],
    )(shifts, w_bwd, resid_all)
    gradient = own + passed_along(upper, "gy", 1)
    entries = angles * rows * depth * lax.axis_size("gy") * lax.axis_size("gz")
    misfit = lax.psum(jnp.sum(resid_share * resid_share), ("gx", "gy", "gz")) / entries
    return (gradient, resid_share, misfit)


def solution(mesh):
    in_specs = (P("gx", "gy", "gz"), P(None, None, "gx"), P(None, "gx"), P("gx", "gy", "gz"))
    out_specs = (P("gx", "gy", "gz"), P("gx", "gy", "gz"), P())
    return jax.shard_map(body, mesh=mesh, in_specs=in_specs, out_specs=out_specs, check_vma=False)
```

```python
import functools

import jax
import jax.numpy as jnp
from jax import lax
from jax.experimental import pallas as pl
from jax.experimental.pallas import tpu as pltpu
from jax.sharding import PartitionSpec as P

SUB = 8
WIN = 16
CHUNK = 2
SKEW = 2
PIECE = 2
MESH = pl.DeviceIdType.MESH


def split(x):
    hi = x.astype(jnp.bfloat16)
    lo = (x - hi.astype(jnp.float32)).astype(jnp.bfloat16)
    return hi, lo


def toeplitz(flat):
    lead, lanes = flat.shape
    wide = jnp.broadcast_to(flat[:, None, :], (lead, SUB, lanes))
    rolled = pltpu.roll(wide, 0, 2, stride=1, stride_axis=1)
    return rolled.reshape(lead * SUB, lanes)


def dot(x, y):
    return jnp.dot(x, y, preferred_element_type=jnp.float32)


def kernel(
    off_ref, wf_ref, wb_ref, vol_ref, meas_ref, grad_ref, resid_ref, mis_ref,
    ext, q, part, fhi, flo, bhi, blo, rbuf, lin, rin, sr, sl, rext, rhs, up, gbuf, mx, my, mz,
    halo_sem, swap_s, swap_r, right_s, right_r, left_s, left_r, tot_s, tot_r, grad_s, grad_r,
    mx_s, mx_r, my_s, my_r, mz_s, mz_r,
):
    cols, rows, depth = vol_ref.shape
    angles = wf_ref.shape[0]
    share = meas_ref.shape[0]
    taps = WIN - SUB
    sizes = {axis: lax.axis_size(axis) for axis in ("gx", "gy", "gz")}
    at_axis = {axis: lax.axis_index(axis) for axis in ("gx", "gy", "gz")}
    gx, gy = at_axis["gx"], at_axis["gy"]
    chips = sizes["gx"] // 2
    z, core = gx // 2, gx % 2
    partner = gx + 1 - 2 * core
    last_y = sizes["gy"] - 1
    chunks = angles // (2 * CHUNK)

    def remote(src, dst, send, recv, axis, to):
        return pltpu.make_async_remote_copy(
            src_ref=src, dst_ref=dst, send_sem=send, recv_sem=recv,
            device_id={axis: to}, device_id_type=MESH,
        )

    barrier = pltpu.get_barrier_semaphore()
    total_peers = 0
    for axis, size in sizes.items():
        for step in range(1, size):
            to = lax.rem(at_axis[axis] + step, size)
            pl.semaphore_signal(barrier, inc=1, device_id={axis: to}, device_id_type=MESH)
        total_peers += size - 1
    pl.semaphore_wait(barrier, total_peers)

    halo = remote(
        vol_ref, ext.at[:, pl.ds(rows, rows), :], halo_sem.at[0], halo_sem.at[1], "gy",
        lax.rem(gy + last_y, last_y + 1),
    )

    @pl.when(gy > 0)
    def _():
        halo.start()

    @pl.when(gy == last_y)
    def _():
        ext[:, rows : 2 * rows] = jnp.zeros((cols, rows, depth), jnp.float32)

    ext[:, :rows] = vol_ref[...]
    ext[:, 2 * rows :] = jnp.zeros((cols, SUB, depth), jnp.float32)
    fhi[...], flo[...] = split(toeplitz(wf_ref[...]))
    bhi[...], blo[...] = split(toeplitz(wb_ref[...]))
    rext[:, :rows] = jnp.zeros((angles, rows, depth), jnp.float32)
    rext[:, 2 * rows :] = jnp.zeros((angles, rows + SUB, depth), jnp.float32)

    @pl.when(z == 0)
    def _():
        lin[...] = jnp.zeros_like(lin)

    @pl.when(z == chips - 1)
    def _():
        rin[...] = jnp.zeros_like(rin)

    def forward(j):
        at = pl.multiple_of(j * SUB, SUB)
        hi, lo = split(ext[:, pl.ds(at, WIN), :].reshape(cols * WIN, depth))
        both = dot(fhi[...], jnp.concatenate([hi, lo], axis=1))
        res = both[:, :depth] + both[:, depth:] + dot(flo[...], hi)
        q[:, pl.ds(at, SUB), :] = res.reshape(angles, SUB, depth)

    @pl.loop(0, rows // SUB - 1)
    def _(j):
        forward(j)

    @pl.when(gy < last_y)
    def _():
        halo.wait_recv()

    @pl.loop(rows // SUB - 1, 2 * rows // SUB)
    def _(j):
        forward(j)

    def first_angle(k, side):
        m = k * CHUNK
        return (2 * (m // share) + side) * share + m % share

    def span(k, side):
        return pl.ds(first_angle(k, side), CHUNK)

    def shift(k, side):
        for step in range(CHUNK):
            a = first_angle(k, side) + step
            part[a] = q[a, pl.ds(off_ref[a], rows), :]

    def swap(k):
        return remote(
            part.at[span(k, 1 - core)], rbuf.at[pl.ds(k * CHUNK, CHUNK)],
            swap_s.at[k], swap_r.at[k], "gx", partner,
        )

    @pl.loop(0, chunks)
    def _(k):
        shift(k, 1 - core)
        swap(k).start()

    @pl.loop(0, chunks)
    def _(k):
        shift(k, core)

    mine = pl.ds(gx * share, share)
    part[mine] = part[mine] - meas_ref[...]

    def chunk(k):
        return pl.ds(k * CHUNK, CHUNK)

    def go_right(k):
        return remote(
            sr.at[chunk(k)], lin.at[chunk(k)], right_s.at[k], right_r.at[k], "gx",
            lax.rem(gx + 2, sizes["gx"]),
        )

    def go_left(k):
        return remote(
            sl.at[chunk(k)], rin.at[chunk(k)], left_s.at[k], left_r.at[k], "gx",
            lax.rem(gx + sizes["gx"] - 2, sizes["gx"]),
        )

    def totals(k, side):
        where = rext.at[span(k, side), pl.ds(rows, rows), :]
        return remote(where, where, tot_s.at[k], tot_r.at[k], "gx", partner)

    from_right = chips - 1 - z

    def inside(k):
        return (k >= 0) & (k < chunks)

    @pl.loop(0, chunks + SKEW * (chips - 1))
    def _(t):
        k_add = t - SKEW * jnp.minimum(z, from_right)
        k_right = t - SKEW * z
        k_left = t - SKEW * from_right
        k_total = t - SKEW * jnp.maximum(z, from_right)

        @pl.when(inside(k_add))
        def _():
            swap(k_add).wait_recv()
            part[span(k_add, core)] = part[span(k_add, core)] + rbuf[chunk(k_add)]

        @pl.when(inside(k_right))
        def _():
            @pl.when(z > 0)
            def _():
                go_right(k_right).wait_recv()

            @pl.when(z < chips - 1)
            def _():
                sr[chunk(k_right)] = lin[chunk(k_right)] + part[span(k_right, core)]
                go_right(k_right).start()

        @pl.when(inside(k_left))
        def _():
            @pl.when(z < chips - 1)
            def _():
                go_left(k_left).wait_recv()

            @pl.when(z > 0)
            def _():
                sl[chunk(k_left)] = rin[chunk(k_left)] + part[span(k_left, core)]
                go_left(k_left).start()

        @pl.when(inside(k_total))
        def _():
            k = k_total
            rext[span(k, core), rows : 2 * rows, :] = (
                lin[chunk(k)] + part[span(k, core)] + rin[chunk(k)]
            )
            totals(k, core).start()

    owned = rext[mine, rows : 2 * rows, :]
    resid_ref[...] = owned
    tile = jnp.sum((owned * owned).reshape(share * rows // SUB, SUB, depth), axis=0)

    def spread(buf, send, recv, axis):
        size, me = sizes[axis], at_axis[axis]
        out = []
        for step in range(1, size):
            to = lax.rem(me + step, size)
            out.append(remote(buf.at[me], buf.at[me], send.at[step - 1], recv.at[step - 1], axis, to))
        return out

    def begin(buf, value, copies):
        buf[copies[0]] = value
        for copy in copies[1]:
            copy.start()

    def finish(buf, copies):
        for copy in copies:
            copy.wait()
        return jnp.sum(buf[...], axis=0)

    over_x = spread(mx, mx_s, mx_r, "gx")
    over_y = spread(my, my_s, my_r, "gy")
    over_z = spread(mz, mz_s, mz_r, "gz")
    begin(mx, tile, (at_axis["gx"], over_x))

    @pl.loop(0, chunks)
    def _(k):
        totals(k, 1 - core).wait_recv()

    def backward(j, out_ref, base):
        at = pl.multiple_of(j * SUB, SUB)

        def gather(a, carry):
            start = rows + base + j * SUB - (taps - 1) - off_ref[a]
            hi, lo = split(rext[a, pl.ds(start, WIN), :])
            to = pl.multiple_of(a * WIN, WIN)
            rhs[pl.ds(to, WIN), :depth] = hi
            rhs[pl.ds(to, WIN), depth:] = lo
            return carry

        lax.fori_loop(0, angles, gather, 0, unroll=8)
        both = dot(bhi[...], rhs[...])
        res = both[:, :depth] + both[:, depth:] + dot(blo[...], rhs[:, :depth])
        out_ref[:, pl.ds(at, SUB), :] = res.reshape(cols, SUB, depth)

    tall = PIECE * SUB
    pieces = rows // tall

    def give(p):
        where = pl.ds(pl.multiple_of(p * tall, tall), tall)
        return remote(
            up.at[:, where, :], gbuf.at[:, where, :], grad_s.at[p], grad_r.at[p], "gy",
            lax.rem(gy + 1, last_y + 1),
        )

    @pl.when(gy < last_y)
    def _():
        @pl.loop(0, pieces)
        def _(p):
            @pl.loop(0, PIECE)
            def _(b):
                backward(p * PIECE + b, up, rows)

            give(p).start()

    begin(my, finish(mx, over_x), (at_axis["gy"], over_y))

    @pl.loop(0, rows // SUB // 2)
    def _(j):
        backward(j, grad_ref, 0)

    begin(mz, finish(my, over_y), (at_axis["gz"], over_z))

    @pl.loop(rows // SUB // 2, rows // SUB)
    def _(j):
        backward(j, grad_ref, 0)

    mis_ref[...] = finish(mz, over_z)

    @pl.when(gy > 0)
    def _():
        @pl.loop(0, pieces)
        def _(p):
            give(p).wait_recv()
            where = pl.ds(pl.multiple_of(p * tall, tall), tall)
            grad_ref[:, where, :] = grad_ref[:, where, :] + gbuf[:, where, :]

        halo.wait_send()

    @pl.when(gy < last_y)
    def _():
        @pl.loop(0, pieces)
        def _(p):
            give(p).wait_send()

    @pl.loop(0, chunks)
    def _(k):
        swap(k).wait_send()
        totals(k, core).wait_send()

        @pl.when(z < chips - 1)
        def _():
            go_right(k).wait_send()

        @pl.when(z > 0)
        def _():
            go_left(k).wait_send()


VMEM = pl.BlockSpec(memory_space=pltpu.VMEM)
SMEM = pl.BlockSpec(memory_space=pltpu.SMEM)


def body(volume, weights, offsets, measured):
    cols, rows, depth = volume.shape
    angles, taps, _ = weights.shape
    share = measured.shape[0]
    shifts = offsets[:, 0]
    pad = ((0, 0), (0, 0), (0, WIN - taps))
    w_fwd = jnp.pad(weights.transpose(0, 2, 1), pad).reshape(angles, cols * WIN)
    w_bwd = jnp.pad(weights[:, ::-1].transpose(2, 0, 1), pad).reshape(cols, angles * WIN)
    f32, bf16 = jnp.float32, jnp.bfloat16
    half = angles // 2
    chunks = half // CHUNK
    sizes = [lax.axis_size(axis) for axis in ("gx", "gy", "gz")]
    dma = pltpu.SemaphoreType.DMA
    scratch = [
        pltpu.VMEM((cols, 2 * rows + SUB, depth), f32),
        pltpu.VMEM((angles, 2 * rows, depth), f32),
        pltpu.VMEM((angles, rows, depth), f32),
        pltpu.VMEM((angles * SUB, cols * WIN), bf16),
        pltpu.VMEM((angles * SUB, cols * WIN), bf16),
        pltpu.VMEM((cols * SUB, angles * WIN), bf16),
        pltpu.VMEM((cols * SUB, angles * WIN), bf16),
    ]
    scratch += [pltpu.VMEM((half, rows, depth), f32)] * 5
    scratch += [
        pltpu.VMEM((angles, 3 * rows + SUB, depth), f32),
        pltpu.VMEM((angles * WIN, 2 * depth), bf16),
        pltpu.VMEM((cols, rows, depth), f32),
        pltpu.VMEM((cols, rows, depth), f32),
    ]
    scratch += [pltpu.VMEM((size, SUB, depth), f32) for size in sizes]
    scratch += [dma((2,))]
    scratch += [dma((chunks,))] * 8
    scratch += [dma((rows // (SUB * PIECE),))] * 2
    for size in sizes:
        scratch += [dma((size - 1,))] * 2
    gradient, resid_share, tile = pl.pallas_call(
        kernel,
        out_shape=[
            jax.ShapeDtypeStruct((cols, rows, depth), f32),
            jax.ShapeDtypeStruct((share, rows, depth), f32),
            jax.ShapeDtypeStruct((SUB, depth), f32),
        ],
        in_specs=[SMEM, VMEM, VMEM, VMEM, VMEM],
        out_specs=[VMEM, VMEM, VMEM],
        scratch_shapes=scratch,
        compiler_params=pltpu.CompilerParams(collective_id=0, has_side_effects=True),
    )(shifts, w_fwd, w_bwd, volume, measured)
    entries = angles * rows * depth * sizes[1] * sizes[2]
    misfit = jnp.sum(tile) / entries
    return (gradient, resid_share, misfit)


def solution(mesh):
    in_specs = (P("gx", "gy", "gz"), P(None, None, "gx"), P(None, "gx"), P("gx", "gy", "gz"))
    out_specs = (P("gx", "gy", "gz"), P("gx", "gy", "gz"), P())
    return jax.shard_map(body, mesh=mesh, in_specs=in_specs, out_specs=out_specs, check_vma=False)
```

```python
import functools

import jax
import jax.numpy as jnp
from jax import lax
from jax.experimental import pallas as pl
from jax.experimental.pallas import tpu as pltpu
from jax.sharding import PartitionSpec as P

SUB = 8
WIN = 16
CHUNK = 2
SKEW = 2
LAG = 2
PIECE = 2
GROUP = 16
MESH = pl.DeviceIdType.MESH


def split(x):
    hi = x.astype(jnp.bfloat16)
    lo = (x - hi.astype(jnp.float32)).astype(jnp.bfloat16)
    return hi, lo


def toeplitz(flat):
    lead, lanes = flat.shape
    wide = jnp.broadcast_to(flat[:, None, :], (lead, SUB, lanes))
    rolled = pltpu.roll(wide, 0, 2, stride=1, stride_axis=1)
    return rolled.reshape(lead * SUB, lanes)


def dot(x, y):
    return jnp.dot(x, y, preferred_element_type=jnp.float32)


def kernel(
    off_ref, wf_ref, wb_ref, vol_ref, meas_ref, grad_ref, resid_ref, mis_ref,
    ext, q, part, fhi, flo, bhi, blo, rbuf, lin, rin, sr, sl, rext, near, mx, myz,
    halo_s, halo_r, swap_s, swap_r, right_s, right_r, left_s, left_r, tot_s, tot_r,
    bef_s, bef_r, pass_s, pass_r, mx_s, mx_r, myz_s, myz_r,
):
    cols, rows, depth = vol_ref.shape
    angles = wf_ref.shape[0]
    share = meas_ref.shape[0]
    taps = WIN - SUB
    sizes = {axis: lax.axis_size(axis) for axis in ("gx", "gy", "gz")}
    at_axis = {axis: lax.axis_index(axis) for axis in ("gx", "gy", "gz")}
    gx, gy = at_axis["gx"], at_axis["gy"]
    chips = sizes["gx"] // 2
    z, core = gx // 2, gx % 2
    partner = gx + 1 - 2 * core
    last_y = sizes["gy"] - 1
    chunks = angles // (2 * CHUNK)

    def remote(src, dst, send, recv, to):
        return pltpu.make_async_remote_copy(
            src_ref=src, dst_ref=dst, send_sem=send, recv_sem=recv,
            device_id=to, device_id_type=MESH,
        )

    def ahead(axis, step):
        return lax.rem(at_axis[axis] + step, sizes[axis])

    over_gx = [{"gx": ahead("gx", step)} for step in range(1, sizes["gx"])]
    over_yz = [
        {"gy": ahead("gy", i), "gz": ahead("gz", j)}
        for i in range(sizes["gy"])
        for j in range(sizes["gz"])
        if i or j
    ]
    barrier = pltpu.get_barrier_semaphore()
    for to in over_gx + over_yz:
        pl.semaphore_signal(barrier, inc=1, device_id=to, device_id_type=MESH)
    pl.semaphore_wait(barrier, len(over_gx) + len(over_yz))

    tall = PIECE * SUB
    pieces = rows // tall
    below = {"gy": ahead("gy", last_y)}
    above = {"gy": ahead("gy", 1)}

    def halo(p):
        at = pl.multiple_of(p * tall, tall)
        return remote(
            vol_ref.at[:, pl.ds(at, tall), :], ext.at[:, pl.ds(rows + at, tall), :],
            halo_s.at[p], halo_r.at[p], below,
        )

    @pl.when(gy > 0)
    def _():
        @pl.loop(0, pieces)
        def _(p):
            halo(p).start()

    @pl.when(gy == last_y)
    def _():
        ext[:, rows : 2 * rows] = jnp.zeros((cols, rows, depth), jnp.float32)

    ext[:, :rows] = vol_ref[...]
    ext[:, 2 * rows :] = jnp.zeros((cols, SUB, depth), jnp.float32)
    fhi[...], flo[...] = split(toeplitz(wf_ref[...]))
    span_k = GROUP * WIN
    for g in range(angles // GROUP):
        wide = toeplitz(wb_ref[:, g * span_k : (g + 1) * span_k])
        bhi[g], blo[g] = split(wide)
    near[:, 2 * rows :] = jnp.zeros((GROUP, SUB, depth), jnp.float32)
    grad_ref[...] = jnp.zeros_like(grad_ref)

    @pl.when(gy == 0)
    def _():
        rext[:, :rows] = jnp.zeros((angles, rows, depth), jnp.float32)

    @pl.when(z == 0)
    def _():
        lin[...] = jnp.zeros_like(lin)

    @pl.when(z == chips - 1)
    def _():
        rin[...] = jnp.zeros_like(rin)

    def forward(j):
        at = pl.multiple_of(j * SUB, SUB)
        hi, lo = split(ext[:, pl.ds(at, WIN), :].reshape(cols * WIN, depth))
        both = dot(fhi[...], jnp.concatenate([hi, lo], axis=1))
        res = both[:, :depth] + both[:, depth:] + dot(flo[...], hi)
        q[:, pl.ds(at, SUB), :] = res.reshape(angles, SUB, depth)

    @pl.loop(0, rows // SUB - 1)
    def _(j):
        forward(j)

    @pl.loop(0, pieces)
    def _(p):
        @pl.when(gy < last_y)
        def _():
            halo(p).wait_recv()

        @pl.loop(0, PIECE)
        def _(b):
            forward(rows // SUB - 1 + p * PIECE + b)

    forward(2 * rows // SUB - 1)

    def first_angle(k, side):
        m = k * CHUNK
        return (2 * (m // share) + side) * share + m % share

    def span(k, side):
        return pl.ds(first_angle(k, side), CHUNK)

    def shift(k, side):
        for step in range(CHUNK):
            a = first_angle(k, side) + step
            part[a] = q[a, pl.ds(off_ref[a], rows), :]

    def swap(k):
        return remote(
            part.at[span(k, 1 - core)], rbuf.at[pl.ds(k * CHUNK, CHUNK)],
            swap_s.at[k], swap_r.at[k], {"gx": partner},
        )

    @pl.loop(0, chunks)
    def _(k):
        shift(k, 1 - core)
        swap(k).start()

    @pl.loop(0, chunks)
    def _(k):
        shift(k, core)

    mine = pl.ds(gx * share, share)
    part[mine] = part[mine] - meas_ref[...]

    def chunk(k):
        return pl.ds(k * CHUNK, CHUNK)

    def go_right(k):
        return remote(
            sr.at[chunk(k)], lin.at[chunk(k)], right_s.at[k], right_r.at[k],
            {"gx": ahead("gx", 2)},
        )

    def go_left(k):
        return remote(
            sl.at[chunk(k)], rin.at[chunk(k)], left_s.at[k], left_r.at[k],
            {"gx": ahead("gx", sizes["gx"] - 2)},
        )

    def totals(k, side):
        where = rext.at[span(k, side), pl.ds(rows, rows), :]
        return remote(where, where, tot_s.at[k], tot_r.at[k], {"gx": partner})

    def climb(k):
        return remote(
            rext.at[span(k, core), pl.ds(rows, rows), :], rext.at[span(k, core), pl.ds(0, rows), :],
            bef_s.at[k], bef_r.at[k], above,
        )

    def passed(k, side):
        where = rext.at[span(k, side), pl.ds(0, rows), :]
        return remote(where, where, pass_s.at[k], pass_r.at[k], {"gx": partner})

    def spread(buf, me, send, recv, peers):
        return [
            remote(buf.at[me], buf.at[me], send.at[i], recv.at[i], to)
            for i, to in enumerate(peers)
        ]

    me_yz = gy * sizes["gz"] + at_axis["gz"]
    tiles_x = spread(mx, gx, mx_s, mx_r, over_gx)
    tiles_yz = spread(myz, me_yz, myz_s, myz_r, over_yz)
    per_group = GROUP // (2 * CHUNK)
    per_step = rows // SUB // per_group

    def backward(g, j):
        at = pl.multiple_of(j * SUB, SUB)
        windows = []
        for i in range(GROUP):
            a = g * GROUP + i
            windows.append(near[i, pl.ds(rows + j * SUB - (taps - 1) - off_ref[a], WIN), :])
        hi, lo = split(jnp.concatenate(windows, axis=0))
        both = dot(bhi[g], jnp.concatenate([hi, lo], axis=1))
        res = both[:, :depth] + both[:, depth:] + dot(blo[g], hi)
        grad_ref[:, pl.ds(at, SUB), :] += res.reshape(cols, SUB, depth)

    from_right = chips - 1 - z

    def inside(k):
        return (k >= 0) & (k < chunks)

    far = jnp.maximum(z, from_right)

    @pl.loop(0, chunks + SKEW * (chips - 1) + LAG + 1 + per_group)
    def _(t):
        k_add = t - SKEW * jnp.minimum(z, from_right)
        k_right = t - SKEW * z
        k_left = t - SKEW * from_right
        k_total = t - SKEW * far
        k_before = k_total - LAG
        k_back = k_before - 1 - per_group

        @pl.when(inside(k_add))
        def _():
            swap(k_add).wait_recv()
            part[span(k_add, core)] = part[span(k_add, core)] + rbuf[chunk(k_add)]

        @pl.when(inside(k_right))
        def _():
            @pl.when(z > 0)
            def _():
                go_right(k_right).wait_recv()

            @pl.when(z < chips - 1)
            def _():
                sr[chunk(k_right)] = lin[chunk(k_right)] + part[span(k_right, core)]
                go_right(k_right).start()

        @pl.when(inside(k_left))
        def _():
            @pl.when(z < chips - 1)
            def _():
                go_left(k_left).wait_recv()

            @pl.when(z > 0)
            def _():
                sl[chunk(k_left)] = rin[chunk(k_left)] + part[span(k_left, core)]
                go_left(k_left).start()

        @pl.when(inside(k_total))
        def _():
            k = k_total
            rext[span(k, core), rows : 2 * rows, :] = (
                lin[chunk(k)] + part[span(k, core)] + rin[chunk(k)]
            )
            totals(k, core).start()

            @pl.when(gy < last_y)
            def _():
                climb(k).start()

        @pl.when(k_total == chunks)
        def _():
            owned = rext[mine, rows : 2 * rows, :]
            resid_ref[...] = owned
            mx[gx] = jnp.sum((owned * owned).reshape(share * rows // SUB, SUB, depth), axis=0)
            for copy in tiles_x:
                copy.start()

        @pl.when(inside(k_before) & (gy > 0))
        def _():
            climb(k_before).wait_recv()
            passed(k_before, core).start()

        @pl.when(k_total == chunks + LAG)
        def _():
            for copy in tiles_x:
                copy.wait()
            myz[me_yz] = jnp.sum(mx[...], axis=0)
            for copy in tiles_yz:
                copy.start()

        @pl.when(inside(k_back))
        def _():
            g = k_back // per_group
            step = k_back % per_group

            @pl.when(step == 0)
            def _():
                @pl.loop(0, per_group)
                def _(i):
                    totals(g * per_group + i, 1 - core).wait_recv()

                    @pl.when(gy > 0)
                    def _():
                        passed(g * per_group + i, 1 - core).wait_recv()

                near[:, : 2 * rows] = rext[pl.ds(g * GROUP, GROUP)]

            @pl.loop(0, per_step)
            def _(i):
                backward(g, step * per_step + i)

    for copy in tiles_yz:
        copy.wait()
    entries = angles * rows * depth * sizes["gy"] * sizes["gz"]
    mis_ref[0, 0] = jnp.sum(jnp.sum(myz[...], axis=0)) * (1.0 / entries)

    @pl.when(gy > 0)
    def _():
        @pl.loop(0, pieces)
        def _(p):
            halo(p).wait_send()

        @pl.loop(0, chunks)
        def _(k):
            passed(k, core).wait_send()

    @pl.loop(0, chunks)
    def _(k):
        swap(k).wait_send()
        totals(k, core).wait_send()

        @pl.when(gy < last_y)
        def _():
            climb(k).wait_send()

        @pl.when(z < chips - 1)
        def _():
            go_right(k).wait_send()

        @pl.when(z > 0)
        def _():
            go_left(k).wait_send()


VMEM = pl.BlockSpec(memory_space=pltpu.VMEM)
SMEM = pl.BlockSpec(memory_space=pltpu.SMEM)


def body(volume, weights, offsets, measured):
    cols, rows, depth = volume.shape
    angles, taps, _ = weights.shape
    share = measured.shape[0]
    shifts = offsets[:, 0]
    pad = ((0, 0), (0, 0), (0, WIN - taps))
    w_fwd = jnp.pad(weights.transpose(0, 2, 1), pad).reshape(angles, cols * WIN)
    w_bwd = jnp.pad(weights[:, ::-1].transpose(2, 0, 1), pad).reshape(cols, angles * WIN)
    f32, bf16 = jnp.float32, jnp.bfloat16
    half = angles // 2
    chunks = half // CHUNK
    sizes = [lax.axis_size(axis) for axis in ("gx", "gy", "gz")]
    dma = pltpu.SemaphoreType.DMA
    scratch = [
        pltpu.VMEM((cols, 2 * rows + SUB, depth), f32),
        pltpu.VMEM((angles, 2 * rows, depth), f32),
        pltpu.VMEM((angles, rows, depth), f32),
        pltpu.VMEM((angles * SUB, cols * WIN), bf16),
        pltpu.VMEM((angles * SUB, cols * WIN), bf16),
        pltpu.VMEM((angles // GROUP, cols * SUB, GROUP * WIN), bf16),
        pltpu.VMEM((angles // GROUP, cols * SUB, GROUP * WIN), bf16),
    ]
    scratch += [pltpu.VMEM((half, rows, depth), f32)] * 5
    scratch += [
        pltpu.VMEM((angles, 2 * rows, depth), f32),
        pltpu.VMEM((GROUP, 2 * rows + SUB, depth), f32),
        pltpu.VMEM((sizes[0], SUB, depth), f32),
        pltpu.VMEM((sizes[1] * sizes[2], SUB, depth), f32),
    ]
    scratch += [dma((rows // (SUB * PIECE),))] * 2
    scratch += [dma((chunks,))] * 12
    scratch += [dma((sizes[0] - 1,))] * 2 + [dma((sizes[1] * sizes[2] - 1,))] * 2
    gradient, resid_share, misfit = pl.pallas_call(
        kernel,
        out_shape=[
            jax.ShapeDtypeStruct((cols, rows, depth), f32),
            jax.ShapeDtypeStruct((share, rows, depth), f32),
            jax.ShapeDtypeStruct((1, 1), f32),
        ],
        in_specs=[SMEM, VMEM, VMEM, VMEM, VMEM],
        out_specs=[VMEM, VMEM, SMEM],
        scratch_shapes=scratch,
        compiler_params=pltpu.CompilerParams(collective_id=0, has_side_effects=True),
    )(shifts, w_fwd, w_bwd, volume, measured)
    return (gradient, resid_share, misfit[0, 0])


def solution(mesh):
    in_specs = (P("gx", "gy", "gz"), P(None, None, "gx"), P(None, "gx"), P("gx", "gy", "gz"))
    out_specs = (P("gx", "gy", "gz"), P("gx", "gy", "gz"), P())
    return jax.shard_map(body, mesh=mesh, in_specs=in_specs, out_specs=out_specs, check_vma=False)
```

```python
import functools

import jax
import jax.numpy as jnp
from jax import lax
from jax.experimental import pallas as pl
from jax.experimental.pallas import tpu as pltpu
from jax.sharding import PartitionSpec as P

SUB = 8
WIN = 16
CHUNK = 2
SKEW = 3
LAG = 3
PIECE = 2
GROUP = 16
MESH = pl.DeviceIdType.MESH


def split(x):
    hi = x.astype(jnp.bfloat16)
    lo = (x - hi.astype(jnp.float32)).astype(jnp.bfloat16)
    return hi, lo


def toeplitz(flat):
    lead, lanes = flat.shape
    wide = jnp.broadcast_to(flat[:, None, :], (lead, SUB, lanes))
    rolled = pltpu.roll(wide, 0, 2, stride=1, stride_axis=1)
    return rolled.reshape(lead * SUB, lanes)


def dot(x, y):
    return jnp.dot(x, y, preferred_element_type=jnp.float32)


def kernel(
    off_ref, wf_ref, wb_ref, vol_ref, meas_ref, grad_ref, resid_ref, mis_ref,
    ext, q, part, fhi, flo, bhi, blo, rbuf, lin, rin, sr, sl, rext, near, mx, myz,
    halo_s, halo_r, swap_s, swap_r, right_s, right_r, left_s, left_r, tot_s, tot_r,
    bef_s, bef_r, pass_s, pass_r, mx_s, mx_r, myz_s, myz_r,
):
    cols, rows, depth = vol_ref.shape
    angles = wf_ref.shape[0]
    share = meas_ref.shape[0]
    taps = WIN - SUB
    sizes = {axis: lax.axis_size(axis) for axis in ("gx", "gy", "gz")}
    at_axis = {axis: lax.axis_index(axis) for axis in ("gx", "gy", "gz")}
    gx, gy = at_axis["gx"], at_axis["gy"]
    chips = sizes["gx"] // 2
    z, core = gx // 2, gx % 2
    partner = gx + 1 - 2 * core
    last_y = sizes["gy"] - 1
    chunks = angles // (2 * CHUNK)

    def remote(src, dst, send, recv, to):
        return pltpu.make_async_remote_copy(
            src_ref=src, dst_ref=dst, send_sem=send, recv_sem=recv,
            device_id=to, device_id_type=MESH,
        )

    def ahead(axis, step):
        return lax.rem(at_axis[axis] + step, sizes[axis])

    over_gx = [{"gx": ahead("gx", step)} for step in range(1, sizes["gx"])]
    over_yz = [
        {"gy": ahead("gy", i), "gz": ahead("gz", j)}
        for i in range(sizes["gy"])
        for j in range(sizes["gz"])
        if i or j
    ]
    barrier = pltpu.get_barrier_semaphore()
    for to in over_gx + over_yz:
        pl.semaphore_signal(barrier, inc=1, device_id=to, device_id_type=MESH)
    pl.semaphore_wait(barrier, len(over_gx) + len(over_yz))

    tall = PIECE * SUB
    pieces = rows // tall
    below = {"gy": ahead("gy", last_y)}
    above = {"gy": ahead("gy", 1)}

    def halo(p):
        at = pl.multiple_of(p * tall, tall)
        return remote(
            vol_ref.at[:, pl.ds(at, tall), :], ext.at[:, pl.ds(rows + at, tall), :],
            halo_s.at[p], halo_r.at[p], below,
        )

    @pl.when(gy > 0)
    def _():
        @pl.loop(0, pieces)
        def _(p):
            halo(p).start()

    @pl.when(gy == last_y)
    def _():
        ext[:, rows : 2 * rows] = jnp.zeros((cols, rows, depth), jnp.float32)

    ext[:, :rows] = vol_ref[...]
    ext[:, 2 * rows :] = jnp.zeros((cols, SUB, depth), jnp.float32)
    fhi[...], flo[...] = split(toeplitz(wf_ref[...]))
    span_k = GROUP * WIN
    for g in range(angles // GROUP):
        wide = toeplitz(wb_ref[:, g * span_k : (g + 1) * span_k])
        bhi[g], blo[g] = split(wide)
    near[:, 2 * rows :] = jnp.zeros((GROUP, SUB, depth), jnp.float32)
    grad_ref[...] = jnp.zeros_like(grad_ref)

    @pl.when(gy == 0)
    def _():
        rext[:, :rows] = jnp.zeros((angles, rows, depth), jnp.float32)

    @pl.when(z == 0)
    def _():
        lin[...] = jnp.zeros_like(lin)

    @pl.when(z == chips - 1)
    def _():
        rin[...] = jnp.zeros_like(rin)

    def forward(j):
        at = pl.multiple_of(j * SUB, SUB)
        hi, lo = split(ext[:, pl.ds(at, WIN), :].reshape(cols * WIN, depth))
        both = dot(fhi[...], jnp.concatenate([hi, lo], axis=1))
        res = both[:, :depth] + both[:, depth:] + dot(flo[...], hi)
        q[:, pl.ds(at, SUB), :] = res.reshape(angles, SUB, depth)

    @pl.loop(0, rows // SUB - 1)
    def _(j):
        forward(j)

    @pl.loop(0, pieces)
    def _(p):
        @pl.when(gy < last_y)
        def _():
            halo(p).wait_recv()

        @pl.loop(0, PIECE)
        def _(b):
            forward(rows // SUB - 1 + p * PIECE + b)

    forward(2 * rows // SUB - 1)

    def first_angle(k, side):
        m = k * CHUNK
        return (2 * (m // share) + side) * share + m % share

    def span(k, side):
        return pl.ds(first_angle(k, side), CHUNK)

    def shift(k, side):
        for step in range(CHUNK):
            a = first_angle(k, side) + step
            part[a] = q[a, pl.ds(off_ref[a], rows), :]

    def swap(k):
        return remote(
            part.at[span(k, 1 - core)], rbuf.at[pl.ds(k * CHUNK, CHUNK)],
            swap_s.at[k], swap_r.at[k], {"gx": partner},
        )

    @pl.loop(0, chunks)
    def _(k):
        shift(k, 1 - core)
        swap(k).start()

    @pl.loop(0, chunks)
    def _(k):
        shift(k, core)

    mine = pl.ds(gx * share, share)
    part[mine] = part[mine] - meas_ref[...]

    def chunk(k):
        return pl.ds(k * CHUNK, CHUNK)

    def go_right(k):
        return remote(
            sr.at[chunk(k)], lin.at[chunk(k)], right_s.at[k], right_r.at[k],
            {"gx": ahead("gx", 2)},
        )

    def go_left(k):
        return remote(
            sl.at[chunk(k)], rin.at[chunk(k)], left_s.at[k], left_r.at[k],
            {"gx": ahead("gx", sizes["gx"] - 2)},
        )

    def totals(k, side):
        where = rext.at[span(k, side), pl.ds(rows, rows), :]
        return remote(where, where, tot_s.at[k], tot_r.at[k], {"gx": partner})

    def climb(k):
        return remote(
            rext.at[span(k, core), pl.ds(rows, rows), :], rext.at[span(k, core), pl.ds(0, rows), :],
            bef_s.at[k], bef_r.at[k], above,
        )

    def passed(k, side):
        where = rext.at[span(k, side), pl.ds(0, rows), :]
        return remote(where, where, pass_s.at[k], pass_r.at[k], {"gx": partner})

    def spread(buf, me, send, recv, peers):
        return [
            remote(buf.at[me], buf.at[me], send.at[i], recv.at[i], to)
            for i, to in enumerate(peers)
        ]

    me_yz = gy * sizes["gz"] + at_axis["gz"]
    tiles_x = spread(mx, gx, mx_s, mx_r, over_gx)
    tiles_yz = spread(myz, me_yz, myz_s, myz_r, over_yz)
    per_group = GROUP // (2 * CHUNK)
    per_step = rows // SUB // per_group

    def backward(g, j):
        at = pl.multiple_of(j * SUB, SUB)
        windows = []
        for i in range(GROUP):
            a = g * GROUP + i
            windows.append(near[i, pl.ds(rows + j * SUB - (taps - 1) - off_ref[a], WIN), :])
        hi, lo = split(jnp.concatenate(windows, axis=0))
        both = dot(bhi[g], jnp.concatenate([hi, lo], axis=1))
        res = both[:, :depth] + both[:, depth:] + dot(blo[g], hi)
        grad_ref[:, pl.ds(at, SUB), :] += res.reshape(cols, SUB, depth)

    from_right = chips - 1 - z

    def inside(k):
        return (k >= 0) & (k < chunks)

    far = jnp.maximum(z, from_right)

    @pl.loop(0, chunks + SKEW * (chips - 1) + LAG + 1 + per_group)
    def _(t):
        k_add = t - SKEW * jnp.minimum(z, from_right)
        k_right = t - SKEW * z
        k_left = t - SKEW * from_right
        k_total = t - SKEW * far
        k_before = k_total - LAG
        k_back = k_before - 1 - per_group

        @pl.when(inside(k_add))
        def _():
            swap(k_add).wait_recv()
            part[span(k_add, core)] = part[span(k_add, core)] + rbuf[chunk(k_add)]

        @pl.when(inside(k_right))
        def _():
            @pl.when(z > 0)
            def _():
                go_right(k_right).wait_recv()

            @pl.when(z < chips - 1)
            def _():
                sr[chunk(k_right)] = lin[chunk(k_right)] + part[span(k_right, core)]
                go_right(k_right).start()

        @pl.when(inside(k_left))
        def _():
            @pl.when(z < chips - 1)
            def _():
                go_left(k_left).wait_recv()

            @pl.when(z > 0)
            def _():
                sl[chunk(k_left)] = rin[chunk(k_left)] + part[span(k_left, core)]
                go_left(k_left).start()

        @pl.when(inside(k_total))
        def _():
            k = k_total
            rext[span(k, core), rows : 2 * rows, :] = (
                lin[chunk(k)] + part[span(k, core)] + rin[chunk(k)]
            )
            totals(k, core).start()

            @pl.when(gy < last_y)
            def _():
                climb(k).start()

        @pl.when(k_total == chunks)
        def _():
            owned = rext[mine, rows : 2 * rows, :]
            resid_ref[...] = owned
            mx[gx] = jnp.sum((owned * owned).reshape(share * rows // SUB, SUB, depth), axis=0)
            for copy in tiles_x:
                copy.start()

        @pl.when(inside(k_before) & (gy > 0))
        def _():
            climb(k_before).wait_recv()
            passed(k_before, core).start()

        @pl.when(k_total == chunks + LAG)
        def _():
            for copy in tiles_x:
                copy.wait()
            myz[me_yz] = jnp.sum(mx[...], axis=0)
            for copy in tiles_yz:
                copy.start()

        @pl.when(inside(k_back))
        def _():
            g = k_back // per_group
            step = k_back % per_group

            @pl.when(step == 0)
            def _():
                @pl.loop(0, per_group)
                def _(i):
                    totals(g * per_group + i, 1 - core).wait_recv()

                    @pl.when(gy > 0)
                    def _():
                        passed(g * per_group + i, 1 - core).wait_recv()

                near[:, : 2 * rows] = rext[pl.ds(g * GROUP, GROUP)]

            @pl.loop(0, per_step)
            def _(i):
                backward(g, step * per_step + i)

    for copy in tiles_yz:
        copy.wait()
    entries = angles * rows * depth * sizes["gy"] * sizes["gz"]
    mis_ref[0, 0] = jnp.sum(jnp.sum(myz[...], axis=0)) * (1.0 / entries)

    @pl.when(gy > 0)
    def _():
        @pl.loop(0, pieces)
        def _(p):
            halo(p).wait_send()

        @pl.loop(0, chunks)
        def _(k):
            passed(k, core).wait_send()

    @pl.loop(0, chunks)
    def _(k):
        swap(k).wait_send()
        totals(k, core).wait_send()

        @pl.when(gy < last_y)
        def _():
            climb(k).wait_send()

        @pl.when(z < chips - 1)
        def _():
            go_right(k).wait_send()

        @pl.when(z > 0)
        def _():
            go_left(k).wait_send()


VMEM = pl.BlockSpec(memory_space=pltpu.VMEM)
SMEM = pl.BlockSpec(memory_space=pltpu.SMEM)


def body(volume, weights, offsets, measured):
    cols, rows, depth = volume.shape
    angles, taps, _ = weights.shape
    share = measured.shape[0]
    shifts = offsets[:, 0]
    pad = ((0, 0), (0, 0), (0, WIN - taps))
    w_fwd = jnp.pad(weights.transpose(0, 2, 1), pad).reshape(angles, cols * WIN)
    w_bwd = jnp.pad(weights[:, ::-1].transpose(2, 0, 1), pad).reshape(cols, angles * WIN)
    f32, bf16 = jnp.float32, jnp.bfloat16
    half = angles // 2
    chunks = half // CHUNK
    sizes = [lax.axis_size(axis) for axis in ("gx", "gy", "gz")]
    dma = pltpu.SemaphoreType.DMA
    scratch = [
        pltpu.VMEM((cols, 2 * rows + SUB, depth), f32),
        pltpu.VMEM((angles, 2 * rows, depth), f32),
        pltpu.VMEM((angles, rows, depth), f32),
        pltpu.VMEM((angles * SUB, cols * WIN), bf16),
        pltpu.VMEM((angles * SUB, cols * WIN), bf16),
        pltpu.VMEM((angles // GROUP, cols * SUB, GROUP * WIN), bf16),
        pltpu.VMEM((angles // GROUP, cols * SUB, GROUP * WIN), bf16),
    ]
    scratch += [pltpu.VMEM((half, rows, depth), f32)] * 5
    scratch += [
        pltpu.VMEM((angles, 2 * rows, depth), f32),
        pltpu.VMEM((GROUP, 2 * rows + SUB, depth), f32),
        pltpu.VMEM((sizes[0], SUB, depth), f32),
        pltpu.VMEM((sizes[1] * sizes[2], SUB, depth), f32),
    ]
    scratch += [dma((rows // (SUB * PIECE),))] * 2
    scratch += [dma((chunks,))] * 12
    scratch += [dma((sizes[0] - 1,))] * 2 + [dma((sizes[1] * sizes[2] - 1,))] * 2
    gradient, resid_share, misfit = pl.pallas_call(
        kernel,
        out_shape=[
            jax.ShapeDtypeStruct((cols, rows, depth), f32),
            jax.ShapeDtypeStruct((share, rows, depth), f32),
            jax.ShapeDtypeStruct((1, 1), f32),
        ],
        in_specs=[SMEM, VMEM, VMEM, VMEM, VMEM],
        out_specs=[VMEM, VMEM, SMEM],
        scratch_shapes=scratch,
        compiler_params=pltpu.CompilerParams(collective_id=0, has_side_effects=True),
    )(shifts, w_fwd, w_bwd, volume, measured)
    return (gradient, resid_share, misfit[0, 0])


def solution(mesh):
    in_specs = (P("gx", "gy", "gz"), P(None, None, "gx"), P(None, "gx"), P("gx", "gy", "gz"))
    out_specs = (P("gx", "gy", "gz"), P("gx", "gy", "gz"), P())
    return jax.shard_map(body, mesh=mesh, in_specs=in_specs, out_specs=out_specs, check_vma=False)
```
